32 devices in a mesh: role: 2 (over core), dev: 16 (over z, y, x).
Axes of the slice: x: 2, y: 2, z: 4, core: 2. Of those that a mesh axis runs over, the one named last changes fastest.
Arguments:
- table_rows: bfloat16 [32, 2048, 128], P('dev'), may hold values from -6 to 6
- piece_table: int32 [32], replicated, may hold values from 0 to 25, as said below
- bag_rows: int32 [32, 8192], P('dev'), may hold values from 0 to 2047
- bag_of: int32 [32, 8192], P('dev'), may hold values from 0 to 4095, never falling along the last dimension, each value on 1 to 8 neighbouring positions
- bag_weight: bfloat16 [32, 8192], P('dev'), may hold values from 0.25 to 2
- dense_input: bfloat16 [4096, 128], P('dev'), may hold values from -6 to 6
- labels: float32 [4096], P('dev'), may hold values from 0 to 1
- cross_u: bfloat16 [3456, 512], replicated, may hold values from -0.109375 to 0.109375
- cross_v: bfloat16 [512, 3456], replicated, may hold values from -0.25 to 0.25
- cross_bias: float32 [3456], replicated, may hold values from -3 to 3
- top_w1: bfloat16 [3456, 1024], replicated, may hold values from -0.109375 to 0.109375
- top_b1: float32 [1024], replicated, may hold values from -3 to 3
- out_w: bfloat16 [1024], replicated, may hold values from -0.375 to 0.375
Outputs:
- piece_grads: bfloat16 [16, 256, 32, 128], P(None, 'role', 'dev')
The draws below stay inside these ranges and needn't reach their ends.
Inputs may be any that keep to these rules, and one draw needn't show every extreme that they name: `piece_table`: every one of the 26 tables owns one piece or more. `bag_of`: in each piece the bag numbers never fall along the lookups, and every sample has 1 to 8 lookups in every piece.
All inputs are finite; a program needn't handle non-finite values.
Results may differ from the reference program's by a relative error of at most 0.012.
The reference program's roundings to bfloat16 on the way count: a program that leaves them out, or rounds other values in their place, can miss the bound.
Values may be sent and summed in bfloat16 or wider, within the bound.
A program may use at most 128 MiB of HBM per device.

```python
import math
import jax
import jax.numpy as jnp
import numpy as np
from jax import lax

E = 128
TABLES = 26
RANK = 512
HIDDEN_SIZE = 1024
TOK_DEV = 256
ROWS_PIECE = 2048
MOST = 8
PIECES = 32
BATCH = 4096
LOOKS_PIECE = 8192
WIDTH = 3456
N_DEV = 16


def placement_helper(key):
    key_first = jax.random.fold_in(key, 11)
    key_second = jax.random.fold_in(key, 12)
    key_third = jax.random.fold_in(key, 13)
    leading = jax.random.permutation(key_first, TABLES).astype(jnp.int32)
    surplus = jax.random.randint(key_second, (PIECES - TABLES,), 0, TABLES).astype(jnp.int32)
    assigned = jnp.concatenate([leading, surplus])
    shuffle = jax.random.permutation(key_third, PIECES)
    return assigned[shuffle].astype(jnp.int32)


def draw_piece_table(key, part):
    return placement_helper(key)


def set_ends(values, key, least, top_value):
    dims = values.shape
    spot = [jax.random.randint(jax.random.fold_in(key, axis), (), 0, dims[axis]) for axis in range(len(dims))]
    values = values.at[tuple(spot)].set(least)
    longest = dims.index(max(dims))
    spot[longest] = (spot[longest] + 1) % dims[longest]
    return values.at[tuple(spot)].set(top_value)


def shard_levels(own_key, shape, cuts, smallest, high):
    gain = 1.0
    for axis_at, parts in cuts:
        heights = jax.random.uniform(jax.random.fold_in(jax.random.fold_in(own_key, 6), axis_at), (parts,), jnp.float32, smallest / len(cuts), high / len(cuts))
        gain = gain * jnp.repeat(jnp.exp(heights), shape[axis_at] // parts).reshape((-1,) + (1,) * (len(shape) - 1 - axis_at))
    return gain


def length_profile(amount, total, limit, skew):
    weights = [(1 << 20) // math.isqrt(grade ** skew) + 1 for grade in range(2, amount + 1)]
    rest, given = total - limit - (amount - 1), [1] * (amount - 1)
    while rest > 0:
        free = [i for i in range(amount - 1) if given[i] < limit]
        pool, budget = sum([weights[i] for i in free]), rest
        for i in free:
            extra = min(limit - given[i], max(1, budget * weights[i] // pool), rest)
            given[i] = given[i] + extra
            rest = rest - extra
    return np.array([limit] + given)


def ragged_sizes(stream_key, amount, total, most, lean):
    if amount == 2:
        one = jax.random.randint(stream_key, (), max(1, total - most), min(most, total - 1) + 1)
        return jnp.stack([one, total - one])
    lengths = jnp.asarray(length_profile(amount, total, most, lean), jnp.int32)
    pairs = (amount - 1) // 2
    donor, sink = lengths[1:1 + 2 * pairs:2], lengths[2:2 + 2 * pairs:2]
    margin = jnp.minimum(donor - 1, most - sink)
    passed = jax.random.randint(jax.random.fold_in(stream_key, 1), (pairs,), 0, 1 << 20) % (margin + 1)
    lengths = lengths.at[1:1 + 2 * pairs:2].set(donor - passed).at[2:2 + 2 * pairs:2].set(sink + passed)
    return lengths[jax.random.permutation(jax.random.fold_in(stream_key, 2), amount)]


def normal_values(key, shape, width, reach, split=(), dtype=jnp.bfloat16):
    entries = jax.random.normal(key, shape, jnp.float32) * width
    if len(split) > 0:
        entries = shard_levels(key, shape, split, -0.22, 0.18) * entries
    return jnp.clip(entries, min=-reach, max=reach).astype(dtype)


def setup_inputs(seed: int = 0) -> dict:
    key_list = jax.random.split(jax.random.key(seed), 14)
    return {
        "table_rows": normal_values(key_list[0], (PIECES, ROWS_PIECE, E), 1.0, 6.0, ((0, 16),)),
        "piece_table": draw_piece_table(jax.random.fold_in(key_list[13], 71), 0),
        "bag_rows": set_ends(jax.random.randint(key_list[2], (PIECES, LOOKS_PIECE), 0, ROWS_PIECE), jax.random.fold_in(key_list[2], 1), 0, ROWS_PIECE - 1).astype(jnp.int32),
        "bag_of": jax.vmap(lambda own: jnp.searchsorted(jnp.cumsum(ragged_sizes(own, BATCH, LOOKS_PIECE, MOST, 2)), jnp.arange(LOOKS_PIECE), side="right"))(jax.random.split(key_list[3], PIECES)).reshape((PIECES, LOOKS_PIECE)).astype(jnp.int32),
        "bag_weight": jnp.clip(jnp.exp(math.log(2.0) - 2.0794415 * jax.random.uniform(key_list[4], (PIECES, LOOKS_PIECE), jnp.float32) ** shard_levels(key_list[4], (PIECES, LOOKS_PIECE), ((0, 16),), -0.2, 0.2)), 0.25, 2.0).astype(jnp.bfloat16),
        "dense_input": normal_values(key_list[5], (BATCH, E), 1.0, 6.0, ((0, 16),)),
        "labels": jnp.clip(1.0 * jax.random.uniform(key_list[6], (BATCH,), jnp.float32) ** shard_levels(key_list[6], (BATCH,), ((0, 16),), -0.2, 0.2), 0.0, 1.0),
        "cross_u": normal_values(key_list[7], (WIDTH, RANK), WIDTH ** -0.5, 0.109375),
        "cross_v": normal_values(key_list[8], (RANK, WIDTH), RANK ** -0.5, 0.25),
        "cross_bias": normal_values(key_list[9], (WIDTH,), 0.5, 3.0, (), jnp.float32),
        "top_w1": normal_values(key_list[10], (WIDTH, HIDDEN_SIZE), WIDTH ** -0.5, 0.109375),
        "top_b1": normal_values(key_list[11], (HIDDEN_SIZE,), 0.5, 3.0, (), jnp.float32),
        "out_w": normal_values(key_list[12], (HIDDEN_SIZE,), (HIDDEN_SIZE // 4) ** -0.5, 0.375),
    }


def dense_grads(pooled, dense_in, label_rows, cross_u, cross_v, cross_bias, top_w1, top_b1, out_w):
    row_count = pooled.shape[0]
    embed_width = dense_in.shape[1]
    features = jnp.concatenate([dense_in.astype(jnp.float32)[:, None, :], pooled], axis=1).reshape(row_count, -1)
    low_rank = jnp.dot(features.astype(jnp.bfloat16), cross_u, preferred_element_type=jnp.float32).astype(jnp.bfloat16)
    cross_out = jnp.dot(low_rank, cross_v, preferred_element_type=jnp.float32) + cross_bias
    mixed = (features * cross_out + features).astype(jnp.bfloat16)
    pre_act = jnp.dot(mixed, top_w1, preferred_element_type=jnp.float32) + top_b1
    out_weight = out_w.astype(jnp.float32)
    sig_act = jax.nn.sigmoid(pre_act)
    logits = jnp.sum(pre_act * sig_act * out_weight, axis=1)
    grad_logit = jax.nn.sigmoid(logits) - label_rows
    slope = sig_act * (1.0 + pre_act * (1.0 - sig_act))
    grad_act = (grad_logit[:, None] * out_weight * slope).astype(jnp.bfloat16)
    grad_mixed = jnp.dot(grad_act, top_w1.T, preferred_element_type=jnp.float32)
    grad_cross = (grad_mixed * features).astype(jnp.bfloat16)
    grad_low = jnp.dot(grad_cross, cross_v.T, preferred_element_type=jnp.float32).astype(jnp.bfloat16)
    grad_features = grad_mixed * (cross_out + 1.0) + jnp.dot(grad_low, cross_u.T, preferred_element_type=jnp.float32)
    return grad_features.reshape(row_count, -1, embed_width)[:, 1:, :].astype(jnp.bfloat16)


def reference(table_rows, piece_table, bag_rows, bag_of, bag_weight, dense_input, labels, cross_u, cross_v, cross_bias, top_w1, top_b1, out_w):
    def add_piece(pooled, element):
        piece_rows, table_id, row_ids, bag_ids, weights = element
        picked = piece_rows[row_ids].astype(jnp.float32)
        summed = jax.ops.segment_sum(picked * weights.astype(jnp.float32)[:, None], bag_ids, num_segments=BATCH)
        rounded = lax.optimization_barrier(summed.astype(jnp.bfloat16)).astype(jnp.float32)
        current = lax.dynamic_index_in_dim(pooled, table_id, 1, keepdims=False)
        return lax.dynamic_update_index_in_dim(pooled, current + rounded, table_id, 1), None

    pooled, _ = lax.scan(add_piece, jnp.zeros((BATCH, TABLES, E), jnp.float32), (table_rows, piece_table, bag_rows, bag_of, bag_weight))
    grad_pooled = dense_grads(pooled, dense_input, labels, cross_u, cross_v, cross_bias, top_w1, top_b1, out_w)
    selected = jnp.take(grad_pooled, piece_table, axis=1)
    return selected.reshape(N_DEV, TOK_DEV, PIECES, E)
```

```python
import functools

import jax
import jax.numpy as jnp
from jax import lax
from jax.experimental import pallas as pl
from jax.experimental.pallas import tpu as pltpu
from jax.sharding import PartitionSpec as P

LANES = 128
WINDOW = 2 * LANES
LOW = 256
CHUNKS = 2
NT = (((1,), (1,)), ((), ()))
NN = (((1,), (0,)), ((), ()))


def dot(a, b, dims=NN):
    return lax.dot_general(a, b, dims, preferred_element_type=jnp.float32)


def flip(tile):
    return tile.astype(jnp.float32).T.astype(jnp.bfloat16)


def pick(table, width, ids):
    low_ids = lax.broadcasted_iota(jnp.int32, (LOW, ids.shape[1]), 0)
    low, high = ids % LOW, ids // LOW
    hot = jnp.where(low_ids == low, 1.0, 0.0).astype(jnp.bfloat16)
    picked = dot(table[:width, :], hot)
    for g in range(1, table.shape[0] // width):
        picked = jnp.where(high == g, dot(table[g * width : (g + 1) * width, :], hot), picked)
    return picked.astype(jnp.bfloat16)


def spread_out(bags, scale, rows):
    bag_ids = lax.broadcasted_iota(jnp.int32, (rows, bags.shape[1]), 0)
    return jnp.where(bag_ids == bags, scale, 0.0).astype(jnp.bfloat16)


def plan_kernel(
    tables, owner_ref, bags_ref, rows_hbm, scale_hbm, table_hbm, plan_ref, base_ref, extra_hbm,
    rows_ref, scale_ref, scale_wide, table_ref, flipped, stage, sems,
):
    blocks, pieces, half, width = extra_hbm.shape
    tiles = bags_ref.shape[0]
    rows = half // CHUNKS
    shift = rows.bit_length() - 1
    spares = max(1, owner_ref.shape[0] - tables)
    flags = tables + 2 * spares
    role = lax.axis_index("role")

    @pl.loop(0, tables)
    def _(t):
        plan_ref[t] = -1

    @pl.loop(0, spares)
    def _(e):
        plan_ref[tables + e] = 0
        plan_ref[tables + spares + e] = -1

    def assign(p, used):
        t = owner_ref[p]
        again = plan_ref[t] >= 0

        @pl.when(again)
        def _():
            plan_ref[tables + used] = p
            plan_ref[tables + spares + used] = t

        @pl.when(jnp.logical_not(again))
        def _():
            plan_ref[t] = p

        return used + again.astype(jnp.int32)

    lax.fori_loop(0, owner_ref.shape[0], assign, jnp.int32(0))

    @pl.loop(0, plan_ref.shape[0] - flags)
    def _(i):
        plan_ref[flags + i] = 0

    group = lax.broadcasted_iota(jnp.int32, base_ref.shape, 1)
    edges = (2 * (group // CHUNKS) + role) * half + group % CHUNKS * rows

    ahead = WINDOW // LANES

    def count(t, state):
        base, over = state
        here = bags_ref[t]
        base = base + jnp.where(here[:, LANES - 1 :] < edges, 1, 0)
        same = (here >> shift) == (bags_ref[t + ahead] >> shift)
        return base, jnp.maximum(over, jnp.where(same, 1, 0))

    state = (jnp.zeros(base_ref.shape, jnp.int32), jnp.zeros((pieces, LANES), jnp.int32))
    base, over = lax.fori_loop(0, tiles - ahead, count, state, unroll=True if tiles <= 64 else 8)
    for t in range(tiles - ahead, tiles):
        base = base + jnp.where(bags_ref[t][:, LANES - 1 :] < edges, 1, 0)
    base_ref[...] = jnp.minimum(base, tiles - ahead - 1)

    @pl.when(jnp.max(over) > 0)
    def _():
        loads = [
            pltpu.make_async_copy(rows_hbm, rows_ref, sems.at[0]),
            pltpu.make_async_copy(scale_hbm, scale_ref, sems.at[1]),
            pltpu.make_async_copy(table_hbm, table_ref, sems.at[2]),
        ]
        for load in loads:
            load.start()
        for load in loads:
            load.wait()
        scale_wide[...] = scale_ref[...].astype(jnp.float32)
        for p in range(pieces):
            for g in range(table_ref.shape[1] // LOW):
                flipped[p, g * width : (g + 1) * width, :] = flip(table_ref[p, g * LOW : (g + 1) * LOW, :])

        for p in range(pieces):

            @pl.loop(0, blocks * CHUNKS)
            def _(e):
                k, c = e // CHUNKS, e % CHUNKS
                edge = (2 * k + role) * half + c * rows
                bags = bags_ref[:, p, :]
                first = jnp.sum(jnp.where(bags < edge, 1, 0))
                last = jnp.sum(jnp.where(bags < edge + rows, 1, 0))
                begin = first // LANES

                def more(t, acc):
                    picked = pick(flipped[p], width, rows_ref[t, p : p + 1, :])
                    spread = spread_out(bags_ref[t, p : p + 1, :] - edge, scale_wide[t, p : p + 1, :], rows)
                    return acc + dot(spread, picked, NT)

                @pl.when(last - first > WINDOW)
                def _():
                    plan_ref[flags + (k * pieces + p) * CHUNKS + c] = 1
                    end = (last + LANES - 1) // LANES
                    acc = lax.fori_loop(begin, end, more, jnp.zeros((rows, width), jnp.float32))
                    stage[...] = acc.astype(jnp.bfloat16)
                    put = pltpu.make_async_copy(
                        stage, extra_hbm.at[k, p, pl.ds(pl.multiple_of(c * rows, rows), rows), :], sems.at[0]
                    )
                    put.start()
                    put.wait()


def plan(piece_table, table_rows, bag_rows, bag_of, bag_weight, half, blocks, tables):
    pieces, length, width = table_rows.shape
    spares = max(1, piece_table.shape[0] - tables)
    lanes = -(-blocks * CHUNKS // LANES) * LANES
    vmem = pl.BlockSpec(memory_space=pltpu.VMEM)
    smem = pl.BlockSpec(memory_space=pltpu.SMEM)
    hbm = pl.BlockSpec(memory_space=pltpu.HBM)
    return pl.pallas_call(
        functools.partial(plan_kernel, tables),
        out_shape=[
            jax.ShapeDtypeStruct((tables + 2 * spares + blocks * pieces * CHUNKS,), jnp.int32),
            jax.ShapeDtypeStruct((pieces, lanes), jnp.int32),
            jax.ShapeDtypeStruct((blocks, pieces, half, width), jnp.bfloat16),
        ],
        in_specs=[smem, vmem, hbm, hbm, hbm],
        out_specs=[smem, vmem, hbm],
        scratch_shapes=[
            pltpu.VMEM(bag_rows.shape, jnp.int32),
            pltpu.VMEM(bag_weight.shape, jnp.bfloat16),
            pltpu.VMEM(bag_weight.shape, jnp.float32),
            pltpu.VMEM(table_rows.shape, jnp.bfloat16),
            pltpu.VMEM((pieces, length // LOW * width, LOW), jnp.bfloat16),
            pltpu.VMEM((half // CHUNKS, width), jnp.bfloat16),
            pltpu.SemaphoreType.DMA((3,)),
        ],
        compiler_params=pltpu.CompilerParams(vmem_limit_bytes=60 * 1024 * 1024),
    )(piece_table, bag_of, bag_rows, bag_weight, table_rows)


def step_kernel(
    plan_ref, base_ref, owner_ref, dense_ref, label_ref, bias_ref, b1_ref, out_w_ref,
    bags_hbm, rows_hbm, scale_hbm, table_hbm, extra_hbm, u_hbm, v_hbm, w_hbm, out_ref,
    bags_ref, rows_ref, scale_ref, scale_wide, table_ref, flipped, extra_ref, pooled,
    u_ref, v_ref, w_ref, feats, crossed, mixed_grad, grads, arrived, outgoing,
    sems, there_send, there_recv, back_send, back_recv,
):
    devices, local_pieces, half, width = out_ref.shape
    pieces = devices * local_pieces
    rows, wide = feats.shape
    tables = wide // width - 1
    spares = max(1, pieces - tables)
    flags = tables + 2 * spares
    role = lax.axis_index("role")
    me = lax.axis_index("dev")
    small = [
        pltpu.make_async_copy(bags_hbm, bags_ref, sems.at[0]),
        pltpu.make_async_copy(rows_hbm, rows_ref, sems.at[1]),
        pltpu.make_async_copy(scale_hbm, scale_ref, sems.at[2]),
        pltpu.make_async_copy(table_hbm, table_ref, sems.at[3]),
        pltpu.make_async_copy(extra_hbm, extra_ref, sems.at[4]),
    ]
    load_u = pltpu.make_async_copy(u_hbm, u_ref, sems.at[5])
    load_v = pltpu.make_async_copy(v_hbm, v_ref, sems.at[6])
    load_w = pltpu.make_async_copy(w_hbm, w_ref, sems.at[7])
    barrier = pltpu.get_barrier_semaphore()

    for load in small:
        load.start()

    @pl.loop(1, devices)
    def _(s):
        pl.semaphore_signal(
            barrier, inc=1, device_id={"dev": (me + s) % devices}, device_id_type=pl.DeviceIdType.MESH
        )

    load_u.start()
    load_v.start()
    load_w.start()

    def partner(s):
        if devices & (devices - 1):
            return (me + s) % devices
        peer = 0
        for b in range(devices.bit_length() - 1):
            bit = 1 << b
            peer = peer + bit * ((me // bit + s // bit) % 2)
        return peer

    def there(c, s):
        peer = partner(s)
        return pltpu.make_async_remote_copy(
            src_ref=pooled.at[peer, :, c * rows : (c + 1) * rows, :],
            dst_ref=arrived[c].at[me],
            send_sem=there_send.at[c, s],
            recv_sem=there_recv.at[c, s],
            device_id={"dev": peer},
            device_id_type=pl.DeviceIdType.MESH,
        )

    def back(c, s):
        peer = partner(s)
        return pltpu.make_async_remote_copy(
            src_ref=outgoing[c].at[peer],
            dst_ref=out_ref.at[me, :, c * rows : (c + 1) * rows, :],
            send_sem=back_send.at[c, s],
            recv_sem=back_recv.at[c, s],
            device_id={"dev": peer},
            device_id_type=pl.DeviceIdType.MESH,
        )

    for load in small:
        load.wait()
    scale_wide[...] = scale_ref[...].astype(jnp.float32)
    for p in range(local_pieces):
        for g in range(table_ref.shape[1] // LOW):
            flipped[p, g * width : (g + 1) * width, :] = flip(table_ref[p, g * LOW : (g + 1) * LOW, :])

    def window(k, p, c):
        edge = (2 * k + role) * half + c * rows
        at = base_ref[p, k * CHUNKS + c]

        def tiles(ref):
            return [ref[at + j, p : p + 1, :] for j in range(WINDOW // LANES + 1)]

        bags = tiles(bags_ref)
        early = bags[0] < edge

        def lay(parts):
            return jnp.concatenate([jnp.where(early, parts[-1], parts[0])] + parts[1:-1], axis=1)

        picked = pick(flipped[p], width, lay(tiles(rows_ref)))
        summed = dot(spread_out(lay(bags) - edge, lay(tiles(scale_wide)), rows), picked, NT)
        flag = jnp.zeros((rows, width), jnp.int32) + plan_ref[flags + (k * local_pieces + p) * CHUNKS + c]
        other = extra_ref[k, p, c * rows : (c + 1) * rows, :].astype(jnp.float32)
        return jnp.where(flag > 0, other, summed).astype(jnp.bfloat16)

    for c in range(CHUNKS):

        @pl.loop(0, devices)
        def _(i):
            k = partner(devices - 1 - i)
            sums = [window(k, p, c) for p in range(local_pieces)]
            for p in range(local_pieces):
                pooled[k, p, c * rows : (c + 1) * rows, :] = sums[p]

            if c == 0:

                @pl.when(i == 1)
                def _():
                    pl.semaphore_wait(barrier, devices - 1)

            @pl.when(i > 0)
            def _():
                there(c, devices - i).start()

        arrived[c][me] = pooled[me, :, c * rows : (c + 1) * rows, :]

    step = next(n for n in (3 * width, width) if wide % n == 0)
    parts = [slice(i, i + step) for i in range(0, wide, step)]
    out_weight = out_w_ref[...].astype(jnp.float32)[None, :]
    row_at = lax.broadcasted_iota(jnp.int32, (rows, 2 * half), 0)
    column_at = lax.broadcasted_iota(jnp.int32, (rows, 2 * half), 1)

    for c in range(CHUNKS):
        feats[:, :width] = dense_ref[pl.ds(pl.multiple_of(role * half + c * rows, rows), rows), :].astype(jnp.float32)

        @pl.loop(1, devices)
        def _(s):
            there(c, s).wait_recv()

        def piece(index):
            return arrived[c][index // local_pieces, index % local_pieces].astype(jnp.float32)

        @pl.loop(0, tables)
        def _(t):
            def add(e, acc):
                own = plan_ref[tables + spares + e] == t
                return acc + piece(plan_ref[tables + e]) * jnp.where(own, 1.0, 0.0)

            acc = piece(plan_ref[t])
            if spares <= 16:
                for e in range(spares):
                    acc = add(e, acc)
            else:
                acc = lax.fori_loop(0, spares, add, acc)
            feats[:, pl.ds(pl.multiple_of((t + 1) * width, width), width)] = acc

        if c == 0:
            load_u.wait()
        low_rank = dot(feats[...].astype(jnp.bfloat16), u_ref[...]).astype(jnp.bfloat16)
        if c == 0:
            load_v.wait()
            load_w.wait()
        pre_act = b1_ref[...][None, :]
        for part in parts:
            cross_out = dot(low_rank, v_ref[:, part]) + bias_ref[part][None, :]
            crossed[:, part] = cross_out
            own = feats[:, part]
            pre_act = pre_act + dot((own * cross_out + own).astype(jnp.bfloat16), w_ref[part, :])
        sig_act = jax.nn.sigmoid(pre_act)
        logits = jnp.sum(pre_act * sig_act * out_weight, axis=1, keepdims=True)
        labels = jnp.sum(
            jnp.where(row_at + (role * half + c * rows) == column_at, label_ref[...][None, :], 0.0),
            axis=1,
            keepdims=True,
        )
        grad_logit = jax.nn.sigmoid(logits) - labels
        slope = sig_act * (1.0 + pre_act * (1.0 - sig_act))
        grad_act = (grad_logit * out_weight * slope).astype(jnp.bfloat16)
        grad_low = jnp.zeros((rows, u_ref.shape[1]), jnp.float32)
        for part in parts:
            grad_mixed = dot(grad_act, w_ref[part, :], NT)
            grad_cross = (grad_mixed * feats[:, part]).astype(jnp.bfloat16)
            mixed_grad[:, part] = grad_mixed * (crossed[:, part] + 1.0)
            grad_low = grad_low + dot(grad_cross, v_ref[:, part], NT)
        grad_low = grad_low.astype(jnp.bfloat16)
        for part in parts:
            whole = (mixed_grad[:, part] + dot(grad_low, u_ref[part, :], NT)).astype(jnp.bfloat16)
            for i in range(step // width):
                grads[part.start // width + i] = whole[:, i * width : (i + 1) * width]

        @pl.loop(0, devices)
        def _(d):
            for i in range(local_pieces):
                outgoing[c][d, i] = grads[owner_ref[d * local_pieces + i] + 1]

        @pl.loop(1, devices)
        def _(i):
            back(c, devices - i).start()

        out_ref[me, :, c * rows : (c + 1) * rows, :] = outgoing[c][me]

    for c in range(CHUNKS):

        @pl.loop(1, devices)
        def _(s):
            there(c, s).wait_send()
            back(c, s).wait_send()
            back(c, s).wait_recv()


def local(
    table_rows, piece_table, bag_rows, bag_of, bag_weight, dense_input, labels,
    cross_u, cross_v, cross_bias, top_w1, top_b1, out_w,
):
    devices = lax.axis_size("dev")
    local_pieces, length, width = table_rows.shape
    half = dense_input.shape[0] // 2
    rows = half // CHUNKS
    wide = cross_u.shape[0]
    tables = wide // width - 1

    def tiled(array):
        return array.reshape(local_pieces, -1, LANES).transpose(1, 0, 2)

    bag_rows, bag_of, bag_weight = tiled(bag_rows), tiled(bag_of), tiled(bag_weight)
    plans, base, extra = plan(piece_table, table_rows, bag_rows, bag_of, bag_weight, half, devices, tables)
    vmem = pl.BlockSpec(memory_space=pltpu.VMEM)
    smem = pl.BlockSpec(memory_space=pltpu.SMEM)
    hbm = pl.BlockSpec(memory_space=pltpu.HBM)
    shape = (devices, local_pieces, half, width)
    block = pltpu.VMEM((devices, local_pieces, rows, width), jnp.bfloat16)
    returned = pl.pallas_call(
        step_kernel,
        out_shape=jax.ShapeDtypeStruct(shape, jnp.bfloat16),
        in_specs=[smem] * 3 + [vmem] * 5 + [hbm] * 8,
        out_specs=vmem,
        scratch_shapes=[
            pltpu.VMEM(bag_of.shape, jnp.int32),
            pltpu.VMEM(bag_rows.shape, jnp.int32),
            pltpu.VMEM(bag_weight.shape, jnp.bfloat16),
            pltpu.VMEM(bag_weight.shape, jnp.float32),
            pltpu.VMEM(table_rows.shape, jnp.bfloat16),
            pltpu.VMEM((local_pieces, length // LOW * width, LOW), jnp.bfloat16),
            pltpu.VMEM(shape, jnp.bfloat16),
            pltpu.VMEM(shape, jnp.bfloat16),
            pltpu.VMEM(cross_u.shape, jnp.bfloat16),
            pltpu.VMEM(cross_v.shape, jnp.bfloat16),
            pltpu.VMEM(top_w1.shape, jnp.bfloat16),
            pltpu.VMEM((rows, wide), jnp.float32),
            pltpu.VMEM((rows, wide), jnp.float32),
            pltpu.VMEM((rows, wide), jnp.float32),
            pltpu.VMEM((wide // width, rows, width), jnp.bfloat16),
            [block] * CHUNKS,
            [block] * CHUNKS,
            pltpu.SemaphoreType.DMA((8,)),
        ]
        + [pltpu.SemaphoreType.DMA((CHUNKS, devices))] * 4,
        compiler_params=pltpu.CompilerParams(
            vmem_limit_bytes=60 * 1024 * 1024, collective_id=0, has_side_effects=True
        ),
    )(
        plans, base, piece_table, dense_input, labels, cross_bias, top_b1, out_w,
        bag_of, bag_rows, bag_weight, table_rows, extra, cross_u, cross_v, top_w1,
    )
    return returned.transpose(0, 2, 1, 3)


def solution(mesh):
    split, whole = P("dev"), P()
    return jax.shard_map(
        local,
        mesh=mesh,
        in_specs=(split, whole, split, split, split, split, split) + (whole,) * 6,
        out_specs=P(None, "role", "dev", None),
        check_vma=False,
    )
```

```python
import functools

import jax
import jax.numpy as jnp
from jax import lax
from jax.experimental import pallas as pl
from jax.experimental.pallas import tpu as pltpu
from jax.sharding import PartitionSpec as P

LANES = 128
WINDOW = 2 * LANES
LOW = 256
HALVES = 2
TOGETHER = 2
NT = (((1,), (1,)), ((), ()))
NN = (((1,), (0,)), ((), ()))


def dot(a, b, dims=NN):
    return lax.dot_general(a, b, dims, preferred_element_type=jnp.float32)


def flip(tile):
    return tile.astype(jnp.float32).T.astype(jnp.bfloat16)


def pick(table, width, ids):
    low_ids = lax.broadcasted_iota(jnp.int32, (LOW, ids.shape[1]), 0)
    low, high = ids % LOW, ids // LOW
    hot = jnp.where(low_ids == low, 1.0, 0.0).astype(jnp.bfloat16)
    picked = dot(table[:width, :], hot)
    for g in range(1, table.shape[0] // width):
        picked = jnp.where(high == g, dot(table[g * width : (g + 1) * width, :], hot), picked)
    return picked.astype(jnp.bfloat16)


def spread_out(bags, scale, rows):
    bag_ids = lax.broadcasted_iota(jnp.int32, (rows, bags.shape[1]), 0)
    return jnp.where(bag_ids == bags, scale, 0.0).astype(jnp.bfloat16)


def plan_kernel(
    tables, owner_ref, bags_ref, rows_hbm, scale_hbm, table_hbm, plan_ref, base_ref, extra_hbm,
    rows_ref, scale_ref, scale_wide, table_ref, flipped, stage, sems,
):
    blocks, pieces, half, width = extra_hbm.shape
    tiles = bags_ref.shape[0]
    rows = half // HALVES
    shift = rows.bit_length() - 1
    spares = max(1, owner_ref.shape[0] - tables)
    flags = tables + 2 * spares
    role = lax.axis_index("role")

    @pl.loop(0, tables)
    def _(t):
        plan_ref[t] = -1

    @pl.loop(0, spares)
    def _(e):
        plan_ref[tables + e] = 0
        plan_ref[tables + spares + e] = -1

    def assign(p, used):
        t = owner_ref[p]
        again = plan_ref[t] >= 0

        @pl.when(again)
        def _():
            plan_ref[tables + used] = p
            plan_ref[tables + spares + used] = t

        @pl.when(jnp.logical_not(again))
        def _():
            plan_ref[t] = p

        return used + again.astype(jnp.int32)

    lax.fori_loop(0, owner_ref.shape[0], assign, jnp.int32(0))

    @pl.loop(0, plan_ref.shape[0] - flags)
    def _(i):
        plan_ref[flags + i] = 0

    group = lax.broadcasted_iota(jnp.int32, base_ref.shape, 1)
    edges = (2 * (group // HALVES) + role) * half + group % HALVES * rows

    ahead = WINDOW // LANES

    def count(t, state):
        base, over = state
        here = bags_ref[t]
        base = base + jnp.where(here[:, LANES - 1 :] < edges, 1, 0)
        same = (here >> shift) == (bags_ref[t + ahead] >> shift)
        return base, jnp.maximum(over, jnp.where(same, 1, 0))

    state = (jnp.zeros(base_ref.shape, jnp.int32), jnp.zeros((pieces, LANES), jnp.int32))
    base, over = lax.fori_loop(0, tiles - ahead, count, state, unroll=True if tiles <= 64 else 8)
    for t in range(tiles - ahead, tiles):
        base = base + jnp.where(bags_ref[t][:, LANES - 1 :] < edges, 1, 0)
    base_ref[...] = jnp.minimum(base, tiles - ahead - 1)

    @pl.when(jnp.max(over) > 0)
    def _():
        loads = [
            pltpu.make_async_copy(rows_hbm, rows_ref, sems.at[0]),
            pltpu.make_async_copy(scale_hbm, scale_ref, sems.at[1]),
            pltpu.make_async_copy(table_hbm, table_ref, sems.at[2]),
        ]
        for load in loads:
            load.start()
        for load in loads:
            load.wait()
        scale_wide[...] = scale_ref[...].astype(jnp.float32)
        for p in range(pieces):
            for g in range(table_ref.shape[1] // LOW):
                flipped[p, g * width : (g + 1) * width, :] = flip(table_ref[p, g * LOW : (g + 1) * LOW, :])

        for p in range(pieces):

            @pl.loop(0, blocks * HALVES)
            def _(e):
                k, c = e // HALVES, e % HALVES
                edge = (2 * k + role) * half + c * rows
                bags = bags_ref[:, p, :]
                first = jnp.sum(jnp.where(bags < edge, 1, 0))
                last = jnp.sum(jnp.where(bags < edge + rows, 1, 0))
                begin = first // LANES

                def more(t, acc):
                    picked = pick(flipped[p], width, rows_ref[t, p : p + 1, :])
                    spread = spread_out(bags_ref[t, p : p + 1, :] - edge, scale_wide[t, p : p + 1, :], rows)
                    return acc + dot(spread, picked, NT)

                @pl.when(last - first > WINDOW)
                def _():
                    plan_ref[flags + (k * pieces + p) * HALVES + c] = 1
                    end = (last + LANES - 1) // LANES
                    acc = lax.fori_loop(begin, end, more, jnp.zeros((rows, width), jnp.float32))
                    stage[...] = acc.astype(jnp.bfloat16)
                    put = pltpu.make_async_copy(
                        stage, extra_hbm.at[k, p, pl.ds(pl.multiple_of(c * rows, rows), rows), :], sems.at[0]
                    )
                    put.start()
                    put.wait()


def plan(piece_table, table_rows, bag_rows, bag_of, bag_weight, half, blocks, tables):
    pieces, length, width = table_rows.shape
    spares = max(1, piece_table.shape[0] - tables)
    lanes = -(-blocks * HALVES // LANES) * LANES
    vmem = pl.BlockSpec(memory_space=pltpu.VMEM)
    smem = pl.BlockSpec(memory_space=pltpu.SMEM)
    hbm = pl.BlockSpec(memory_space=pltpu.HBM)
    return pl.pallas_call(
        functools.partial(plan_kernel, tables),
        out_shape=[
            jax.ShapeDtypeStruct((tables + 2 * spares + blocks * pieces * HALVES,), jnp.int32),
            jax.ShapeDtypeStruct((pieces, lanes), jnp.int32),
            jax.ShapeDtypeStruct((blocks, pieces, half, width), jnp.bfloat16),
        ],
        in_specs=[smem, vmem, hbm, hbm, hbm],
        out_specs=[smem, vmem, hbm],
        scratch_shapes=[
            pltpu.VMEM(bag_rows.shape, jnp.int32),
            pltpu.VMEM(bag_weight.shape, jnp.bfloat16),
            pltpu.VMEM(bag_weight.shape, jnp.float32),
            pltpu.VMEM(table_rows.shape, jnp.bfloat16),
            pltpu.VMEM((pieces, length // LOW * width, LOW), jnp.bfloat16),
            pltpu.VMEM((half // HALVES, width), jnp.bfloat16),
            pltpu.SemaphoreType.DMA((3,)),
        ],
        compiler_params=pltpu.CompilerParams(vmem_limit_bytes=60 * 1024 * 1024),
    )(piece_table, bag_of, bag_rows, bag_weight, table_rows)


def step_kernel(
    plan_ref, base_ref, owner_ref, dense_ref, label_ref, bias_ref, b1_ref, out_w_ref,
    bags_hbm, rows_hbm, scale_hbm, table_hbm, extra_hbm, u_hbm, v_hbm, w_hbm, out_ref,
    bags_ref, rows_ref, scale_ref, scale_wide, table_ref, flipped, extra_ref, pooled,
    u_ref, v_ref, w_ref, feats, crossed, mixed_grad, grads, arrived, outgoing,
    sems, there_send, there_recv, back_send, back_recv,
):
    devices, local_pieces, half, width = out_ref.shape
    pieces = devices * local_pieces
    rows, wide = feats.shape
    group = half // HALVES
    tables = wide // width - 1
    spares = max(1, pieces - tables)
    flags = tables + 2 * spares
    role = lax.axis_index("role")
    me = lax.axis_index("dev")
    small = [
        pltpu.make_async_copy(bags_hbm, bags_ref, sems.at[0]),
        pltpu.make_async_copy(rows_hbm, rows_ref, sems.at[1]),
        pltpu.make_async_copy(scale_hbm, scale_ref, sems.at[2]),
        pltpu.make_async_copy(table_hbm, table_ref, sems.at[3]),
        pltpu.make_async_copy(extra_hbm, extra_ref, sems.at[4]),
    ]
    load_u = pltpu.make_async_copy(u_hbm, u_ref, sems.at[5])
    load_v = pltpu.make_async_copy(v_hbm, v_ref, sems.at[6])
    load_w = pltpu.make_async_copy(w_hbm, w_ref, sems.at[7])
    barrier = pltpu.get_barrier_semaphore()

    for load in small:
        load.start()

    @pl.loop(1, devices)
    def _(s):
        pl.semaphore_signal(
            barrier, inc=1, device_id={"dev": (me + s) % devices}, device_id_type=pl.DeviceIdType.MESH
        )

    load_u.start()
    load_v.start()
    load_w.start()

    def partner(s):
        if devices & (devices - 1):
            return (me + s) % devices
        peer = 0
        for b in range(devices.bit_length() - 1):
            bit = 1 << b
            peer = peer + bit * ((me // bit + s // bit) % 2)
        return peer

    def there(s):
        peer = partner(s)
        return pltpu.make_async_remote_copy(
            src_ref=pooled.at[peer],
            dst_ref=arrived.at[me],
            send_sem=there_send.at[s],
            recv_sem=there_recv.at[s],
            device_id={"dev": peer},
            device_id_type=pl.DeviceIdType.MESH,
        )

    def back(s):
        peer = partner(s)
        return pltpu.make_async_remote_copy(
            src_ref=outgoing.at[peer],
            dst_ref=out_ref.at[me],
            send_sem=back_send.at[s],
            recv_sem=back_recv.at[s],
            device_id={"dev": peer},
            device_id_type=pl.DeviceIdType.MESH,
        )

    for load in small:
        load.wait()
    scale_wide[...] = scale_ref[...].astype(jnp.float32)
    for p in range(local_pieces):
        for g in range(table_ref.shape[1] // LOW):
            flipped[p, g * width : (g + 1) * width, :] = flip(table_ref[p, g * LOW : (g + 1) * LOW, :])

    def windows(places, p):
        laid = []
        for k, c in places:
            edge = (2 * k + role) * half + c * group
            at = base_ref[p, k * HALVES + c]

            def tiles(ref):
                return [ref[at + j, p : p + 1, :] for j in range(WINDOW // LANES + 1)]

            bags = tiles(bags_ref)
            early = bags[0] < edge

            def lay(tiles):
                return [jnp.where(early, tiles[-1], tiles[0])] + tiles[1:-1]

            laid.append((lay(tiles(rows_ref)), [bag - edge for bag in lay(bags)], lay(tiles(scale_wide))))
        picked = pick(flipped[p], width, jnp.concatenate([tile for ids, _, _ in laid for tile in ids], axis=1))
        sums = []
        for n, (k, c) in enumerate(places):
            bags, scale = (jnp.concatenate(tiles, axis=1) for tiles in laid[n][1:])
            summed = dot(spread_out(bags, scale, group), picked[:, n * WINDOW : (n + 1) * WINDOW], NT)
            flag = jnp.zeros((group, width), jnp.int32) + plan_ref[flags + (k * local_pieces + p) * HALVES + c]
            other = extra_ref[k, p, c * group : (c + 1) * group, :].astype(jnp.float32)
            sums.append(jnp.where(flag > 0, other, summed).astype(jnp.bfloat16))
        return sums

    together = TOGETHER if devices % TOGETHER == 0 else 1

    def send(i):
        for n in range(together):
            s = devices - 1 - (i * together + n)

            @pl.when(s > 0)
            def _():
                there(s).start()

    @pl.loop(0, devices // together)
    def _(i):
        @pl.when(i == 1)
        def _():
            pl.semaphore_wait(barrier, devices - 1)

        @pl.when(i > 0)
        def _():
            send(i - 1)

        places = [(partner(devices - 1 - (i * together + n)), c) for n in range(together) for c in range(HALVES)]
        for p in range(local_pieces):
            for (k, c), summed in zip(places, windows(places, p)):
                pooled[k, p, c * group : (c + 1) * group, :] = summed

    arrived[me] = pooled[me]
    send(devices // together - 1)

    step = next(n for n in (3 * width, width) if wide % n == 0)
    parts = [slice(i, i + step) for i in range(0, wide, step)]
    out_weight = out_w_ref[...].astype(jnp.float32)[None, :]
    row_at = lax.broadcasted_iota(jnp.int32, (rows, 2 * half), 0)
    column_at = lax.broadcasted_iota(jnp.int32, (rows, 2 * half), 1)

    feats[:, :width] = dense_ref[pl.ds(pl.multiple_of(role * half, half), half), :].astype(jnp.float32)

    @pl.loop(1, devices)
    def _(s):
        there(s).wait_recv()

    def piece(index):
        return arrived[index // local_pieces, index % local_pieces].astype(jnp.float32)

    @pl.loop(0, tables)
    def _(t):
        def add(e, acc):
            own = plan_ref[tables + spares + e] == t
            return acc + piece(plan_ref[tables + e]) * jnp.where(own, 1.0, 0.0)

        acc = piece(plan_ref[t])
        if spares <= 16:
            for e in range(spares):
                acc = add(e, acc)
        else:
            acc = lax.fori_loop(0, spares, add, acc)
        feats[:, pl.ds(pl.multiple_of((t + 1) * width, width), width)] = acc

    load_u.wait()
    low_rank = dot(feats[...].astype(jnp.bfloat16), u_ref[...]).astype(jnp.bfloat16)
    load_v.wait()
    load_w.wait()
    pre_act = b1_ref[...][None, :]
    for part in parts:
        cross_out = dot(low_rank, v_ref[:, part]) + bias_ref[part][None, :]
        crossed[:, part] = cross_out
        own = feats[:, part]
        pre_act = pre_act + dot((own * cross_out + own).astype(jnp.bfloat16), w_ref[part, :])
    sig_act = jax.nn.sigmoid(pre_act)
    logits = jnp.sum(pre_act * sig_act * out_weight, axis=1, keepdims=True)
    labels = jnp.sum(
        jnp.where(row_at + (role * half) == column_at, label_ref[...][None, :], 0.0),
        axis=1,
        keepdims=True,
    )
    grad_logit = jax.nn.sigmoid(logits) - labels
    slope = sig_act * (1.0 + pre_act * (1.0 - sig_act))
    grad_act = (grad_logit * out_weight * slope).astype(jnp.bfloat16)
    grad_low = jnp.zeros((rows, u_ref.shape[1]), jnp.float32)
    for part in parts:
        grad_mixed = dot(grad_act, w_ref[part, :], NT)
        grad_cross = (grad_mixed * feats[:, part]).astype(jnp.bfloat16)
        mixed_grad[:, part] = grad_mixed * (crossed[:, part] + 1.0)
        grad_low = grad_low + dot(grad_cross, v_ref[:, part], NT)
    grad_low = grad_low.astype(jnp.bfloat16)
    for part in parts:
        whole = (mixed_grad[:, part] + dot(grad_low, u_ref[part, :], NT)).astype(jnp.bfloat16)
        for i in range(step // width):
            grads[part.start // width + i] = whole[:, i * width : (i + 1) * width]

    @pl.loop(0, devices)
    def _(i):
        d = partner(devices - 1 - i)
        for p in range(local_pieces):
            outgoing[d, p] = grads[owner_ref[d * local_pieces + p] + 1]

        @pl.when(i > 0)
        def _():
            back(devices - i).start()

    out_ref[me] = outgoing[me]

    @pl.loop(1, devices)
    def _(s):
        there(s).wait_send()
        back(s).wait_send()
        back(s).wait_recv()


def local(
    table_rows, piece_table, bag_rows, bag_of, bag_weight, dense_input, labels,
    cross_u, cross_v, cross_bias, top_w1, top_b1, out_w,
):
    devices = lax.axis_size("dev")
    local_pieces, length, width = table_rows.shape
    half = dense_input.shape[0] // 2
    wide = cross_u.shape[0]
    tables = wide // width - 1

    def tiled(array):
        return array.reshape(local_pieces, -1, LANES).transpose(1, 0, 2)

    bag_rows, bag_of, bag_weight = tiled(bag_rows), tiled(bag_of), tiled(bag_weight)
    plans, base, extra = plan(piece_table, table_rows, bag_rows, bag_of, bag_weight, half, devices, tables)
    vmem = pl.BlockSpec(memory_space=pltpu.VMEM)
    smem = pl.BlockSpec(memory_space=pltpu.SMEM)
    hbm = pl.BlockSpec(memory_space=pltpu.HBM)
    shape = (devices, local_pieces, half, width)
    returned = pl.pallas_call(
        step_kernel,
        out_shape=jax.ShapeDtypeStruct(shape, jnp.bfloat16),
        in_specs=[smem] * 3 + [vmem] * 5 + [hbm] * 8,
        out_specs=vmem,
        scratch_shapes=[
            pltpu.VMEM(bag_of.shape, jnp.int32),
            pltpu.VMEM(bag_rows.shape, jnp.int32),
            pltpu.VMEM(bag_weight.shape, jnp.bfloat16),
            pltpu.VMEM(bag_weight.shape, jnp.float32),
            pltpu.VMEM(table_rows.shape, jnp.bfloat16),
            pltpu.VMEM((local_pieces, length // LOW * width, LOW), jnp.bfloat16),
            pltpu.VMEM(shape, jnp.bfloat16),
            pltpu.VMEM(shape, jnp.bfloat16),
            pltpu.VMEM(cross_u.shape, jnp.bfloat16),
            pltpu.VMEM(cross_v.shape, jnp.bfloat16),
            pltpu.VMEM(top_w1.shape, jnp.bfloat16),
            pltpu.VMEM((half, wide), jnp.float32),
            pltpu.VMEM((half, wide), jnp.float32),
            pltpu.VMEM((half, wide), jnp.float32),
            pltpu.VMEM((wide // width, half, width), jnp.bfloat16),
            pltpu.VMEM(shape, jnp.bfloat16),
            pltpu.VMEM(shape, jnp.bfloat16),
            pltpu.SemaphoreType.DMA((8,)),
        ]
        + [pltpu.SemaphoreType.DMA((devices,))] * 4,
        compiler_params=pltpu.CompilerParams(
            vmem_limit_bytes=60 * 1024 * 1024, collective_id=0, has_side_effects=True
        ),
    )(
        plans, base, piece_table, dense_input, labels, cross_bias, top_b1, out_w,
        bag_of, bag_rows, bag_weight, table_rows, extra, cross_u, cross_v, top_w1,
    )
    return returned.transpose(0, 2, 1, 3)


def solution(mesh):
    split, whole = P("dev"), P()
    return jax.shard_map(
        local,
        mesh=mesh,
        in_specs=(split, whole, split, split, split, split, split) + (whole,) * 6,
        out_specs=P(None, "role", "dev", None),
        check_vma=False,
    )
```

```python
import functools

import jax
import jax.numpy as jnp
from jax import lax
from jax.experimental import pallas as pl
from jax.experimental.pallas import tpu as pltpu
from jax.sharding import PartitionSpec as P

LANES = 128
WINDOW = 2 * LANES
LOW = 256
CHUNKS = 2
TOGETHER = 4
NT = (((1,), (1,)), ((), ()))
NN = (((1,), (0,)), ((), ()))


def dot(a, b, dims=NN):
    return lax.dot_general(a, b, dims, preferred_element_type=jnp.float32)


def flip(tile):
    return tile.astype(jnp.float32).T.astype(jnp.bfloat16)


def pick(table, width, ids):
    low_ids = lax.broadcasted_iota(jnp.int32, (LOW, ids.shape[1]), 0)
    low, high = ids % LOW, ids // LOW
    hot = jnp.where(low_ids == low, 1.0, 0.0).astype(jnp.bfloat16)
    picked = dot(table[:width, :], hot)
    for g in range(1, table.shape[0] // width):
        picked = jnp.where(high == g, dot(table[g * width : (g + 1) * width, :], hot), picked)
    return picked.astype(jnp.bfloat16)


def spread_out(bags, scale, rows):
    bag_ids = lax.broadcasted_iota(jnp.int32, (rows, bags.shape[1]), 0)
    return jnp.where(bag_ids == bags, scale, 0.0).astype(jnp.bfloat16)


def plan_kernel(
    tables, owner_ref, bags_hbm, rows_hbm, scale_hbm, table_hbm, plan_ref, base_ref, extra_hbm,
    bags_ref, rows_ref, scale_ref, scale_wide, table_ref, flipped, stage, sems,
):
    blocks, pieces, half, width = extra_hbm.shape
    tiles = bags_ref.shape[0]
    rows = half // CHUNKS
    shift = rows.bit_length() - 1
    spares = max(1, owner_ref.shape[0] - tables)
    flags = tables + 2 * spares
    owners = flags + blocks * pieces * CHUNKS
    role = lax.axis_index("role")
    load_bags = pltpu.make_async_copy(bags_hbm, bags_ref, sems.at[3])
    load_bags.start()

    @pl.loop(0, tables)
    def _(t):
        plan_ref[t] = -1

    @pl.loop(0, spares)
    def _(e):
        plan_ref[tables + e] = 0
        plan_ref[tables + spares + e] = -1

    def assign(p, used):
        t = owner_ref[p]
        plan_ref[owners + p] = t
        again = plan_ref[t] >= 0

        @pl.when(again)
        def _():
            plan_ref[tables + used] = p
            plan_ref[tables + spares + used] = t

        @pl.when(jnp.logical_not(again))
        def _():
            plan_ref[t] = p

        return used + again.astype(jnp.int32)

    lax.fori_loop(0, owner_ref.shape[0], assign, jnp.int32(0))

    @pl.loop(0, owners - flags)
    def _(i):
        plan_ref[flags + i] = 0

    load_bags.wait()

    group = lax.broadcasted_iota(jnp.int32, base_ref.shape, 1)
    edges = (2 * (group // CHUNKS) + role) * half + group % CHUNKS * rows

    ahead = WINDOW // LANES

    def count(t, state):
        base, over = state
        here = bags_ref[t]
        base = base + jnp.where(here[:, LANES - 1 :] < edges, 1, 0)
        same = (here >> shift) == (bags_ref[t + ahead] >> shift)
        return base, jnp.maximum(over, jnp.where(same, 1, 0))

    state = (jnp.zeros(base_ref.shape, jnp.int32), jnp.zeros((pieces, LANES), jnp.int32))
    base, over = lax.fori_loop(0, tiles - ahead, count, state, unroll=True if tiles <= 64 else 8)
    for t in range(tiles - ahead, tiles):
        base = base + jnp.where(bags_ref[t][:, LANES - 1 :] < edges, 1, 0)
    base_ref[...] = jnp.minimum(base, tiles - ahead - 1)

    @pl.when(jnp.max(over) > 0)
    def _():
        loads = [
            pltpu.make_async_copy(rows_hbm, rows_ref, sems.at[0]),
            pltpu.make_async_copy(scale_hbm, scale_ref, sems.at[1]),
            pltpu.make_async_copy(table_hbm, table_ref, sems.at[2]),
        ]
        for load in loads:
            load.start()
        for load in loads:
            load.wait()
        scale_wide[...] = scale_ref[...].astype(jnp.float32)
        for p in range(pieces):
            for g in range(table_ref.shape[1] // LOW):
                flipped[p, g * width : (g + 1) * width, :] = flip(table_ref[p, g * LOW : (g + 1) * LOW, :])

        for p in range(pieces):

            @pl.loop(0, blocks * CHUNKS)
            def _(e):
                k, c = e // CHUNKS, e % CHUNKS
                edge = (2 * k + role) * half + c * rows
                bags = bags_ref[:, p, :]
                first = jnp.sum(jnp.where(bags < edge, 1, 0))
                last = jnp.sum(jnp.where(bags < edge + rows, 1, 0))
                begin = first // LANES

                def more(t, acc):
                    picked = pick(flipped[p], width, rows_ref[t, p : p + 1, :])
                    spread = spread_out(bags_ref[t, p : p + 1, :] - edge, scale_wide[t, p : p + 1, :], rows)
                    return acc + dot(spread, picked, NT)

                @pl.when(last - first > WINDOW)
                def _():
                    plan_ref[flags + (k * pieces + p) * CHUNKS + c] = 1
                    end = (last + LANES - 1) // LANES
                    acc = lax.fori_loop(begin, end, more, jnp.zeros((rows, width), jnp.float32))
                    stage[...] = acc.astype(jnp.bfloat16)
                    put = pltpu.make_async_copy(
                        stage, extra_hbm.at[k, p, pl.ds(pl.multiple_of(c * rows, rows), rows), :], sems.at[0]
                    )
                    put.start()
                    put.wait()


def plan(piece_table, table_rows, bag_rows, bag_of, bag_weight, half, blocks, tables):
    pieces, length, width = table_rows.shape
    spares = max(1, piece_table.shape[0] - tables)
    lanes = -(-blocks * CHUNKS // LANES) * LANES
    entries = tables + 2 * spares + blocks * pieces * CHUNKS + piece_table.shape[0]
    vmem = pl.BlockSpec(memory_space=pltpu.VMEM)
    smem = pl.BlockSpec(memory_space=pltpu.SMEM)
    hbm = pl.BlockSpec(memory_space=pltpu.HBM)
    return pl.pallas_call(
        functools.partial(plan_kernel, tables),
        out_shape=[
            jax.ShapeDtypeStruct((-(-entries // LANES) * LANES,), jnp.int32),
            jax.ShapeDtypeStruct((pieces, lanes), jnp.int32),
            jax.ShapeDtypeStruct((blocks, pieces, half, width), jnp.bfloat16),
        ],
        in_specs=[smem, hbm, hbm, hbm, hbm],
        out_specs=[smem, vmem, hbm],
        scratch_shapes=[
            pltpu.VMEM(bag_of.shape, jnp.int32),
            pltpu.VMEM(bag_rows.shape, jnp.int32),
            pltpu.VMEM(bag_weight.shape, jnp.bfloat16),
            pltpu.VMEM(bag_weight.shape, jnp.float32),
            pltpu.VMEM(table_rows.shape, jnp.bfloat16),
            pltpu.VMEM((pieces, length // LOW * width, LOW), jnp.bfloat16),
            pltpu.VMEM((half // CHUNKS, width), jnp.bfloat16),
            pltpu.SemaphoreType.DMA((4,)),
        ],
        compiler_params=pltpu.CompilerParams(vmem_limit_bytes=60 * 1024 * 1024),
    )(piece_table, bag_of, bag_rows, bag_weight, table_rows)


def step_kernel(
    plan_hbm, base_hbm, dense_hbm, label_hbm, bias_hbm, b1_hbm, out_w_hbm, bags_hbm, rows_hbm, scale_hbm, table_hbm, extra_hbm, u_hbm, v_hbm, w_hbm, out_ref,
    plan_ref, base_ref, dense_ref, label_ref, bias_ref, b1_ref, out_w_ref,
    bags_ref, rows_ref, scale_ref, scale_wide, table_ref, flipped, extra_ref, pooled,
    u_ref, v_ref, w_ref, feats, crossed, mixed_grad, grads, arrived, outgoing,
    sems, there_send, there_recv, back_send, back_recv,
):
    devices, local_pieces, half, width = out_ref.shape
    pieces = devices * local_pieces
    rows, wide = feats.shape
    tables = wide // width - 1
    spares = max(1, pieces - tables)
    flags = tables + 2 * spares
    owners = flags + devices * local_pieces * CHUNKS
    role = lax.axis_index("role")
    me = lax.axis_index("dev")
    first = [
        (table_hbm, table_ref), (scale_hbm, scale_ref), (bags_hbm, bags_ref), (rows_hbm, rows_ref),
        (plan_hbm, plan_ref), (base_hbm, base_ref), (extra_hbm, extra_ref),
    ]
    later = [
        (dense_hbm, dense_ref), (label_hbm, label_ref), (bias_hbm, bias_ref), (b1_hbm, b1_ref), (out_w_hbm, out_w_ref),
    ]
    loads = [pltpu.make_async_copy(*pair, sems.at[3 + n]) for n, pair in enumerate(first + later)]
    load_u = pltpu.make_async_copy(u_hbm, u_ref, sems.at[0])
    load_v = pltpu.make_async_copy(v_hbm, v_ref, sems.at[1])
    load_w = pltpu.make_async_copy(w_hbm, w_ref, sems.at[2])
    barrier = pltpu.get_barrier_semaphore()

    for load in loads:
        load.start()

    @pl.loop(1, devices)
    def _(s):
        pl.semaphore_signal(
            barrier, inc=1, device_id={"dev": (me + s) % devices}, device_id_type=pl.DeviceIdType.MESH
        )

    load_u.start()
    load_v.start()
    load_w.start()

    def partner(s):
        if devices & (devices - 1):
            return (me + s) % devices
        peer = 0
        for b in range(devices.bit_length() - 1):
            bit = 1 << b
            peer = peer + bit * ((me // bit + s // bit) % 2)
        return peer

    def there(c, s):
        peer = partner(s)
        return pltpu.make_async_remote_copy(
            src_ref=pooled.at[peer, :, c * rows : (c + 1) * rows, :],
            dst_ref=arrived[c].at[me],
            send_sem=there_send.at[c, s],
            recv_sem=there_recv.at[c, s],
            device_id={"dev": peer},
            device_id_type=pl.DeviceIdType.MESH,
        )

    def back(c, s):
        peer = partner(s)
        return pltpu.make_async_remote_copy(
            src_ref=outgoing[c].at[peer],
            dst_ref=out_ref.at[me, :, c * rows : (c + 1) * rows, :],
            send_sem=back_send.at[c, s],
            recv_sem=back_recv.at[c, s],
            device_id={"dev": peer},
            device_id_type=pl.DeviceIdType.MESH,
        )

    loads[0].wait()
    for p in range(local_pieces):
        for g in range(table_ref.shape[1] // LOW):
            flipped[p, g * width : (g + 1) * width, :] = flip(table_ref[p, g * LOW : (g + 1) * LOW, :])
    for load in loads[1 : len(first)]:
        load.wait()
    scale_wide[...] = scale_ref[...].astype(jnp.float32)

    def windows(places, p):
        laid = []
        for k, c in places:
            edge = (2 * k + role) * half + c * rows
            at = base_ref[p, k * CHUNKS + c]

            def tiles(ref):
                return [ref[at + j, p : p + 1, :] for j in range(WINDOW // LANES + 1)]

            bags = tiles(bags_ref)
            early = bags[0] < edge

            def lay(tiles):
                return [jnp.where(early, tiles[-1], tiles[0])] + tiles[1:-1]

            laid.append((lay(tiles(rows_ref)), [bag - edge for bag in lay(bags)], lay(tiles(scale_wide))))
        picked = pick(flipped[p], width, jnp.concatenate([tile for ids, _, _ in laid for tile in ids], axis=1))
        sums = []
        for n, (k, c) in enumerate(places):
            bags, scale = (jnp.concatenate(tiles, axis=1) for tiles in laid[n][1:])
            summed = dot(spread_out(bags, scale, rows), picked[:, n * WINDOW : (n + 1) * WINDOW], NT)
            flag = jnp.zeros((rows, width), jnp.int32) + plan_ref[flags + (k * local_pieces + p) * CHUNKS + c]
            other = extra_ref[k, p, c * rows : (c + 1) * rows, :].astype(jnp.float32)
            sums.append(jnp.where(flag > 0, other, summed).astype(jnp.bfloat16))
        return sums

    together = TOGETHER if devices % TOGETHER == 0 else 1

    def turn(i):
        return devices - 1 - i

    def send(c, i):
        for n in range(together):
            s = turn(i * together + n)

            @pl.when(s > 0)
            def _():
                there(c, s).start()

    for c in range(CHUNKS):

        @pl.loop(0, devices // together)
        def _(i):
            if c == 0:

                @pl.when(i == 1)
                def _():
                    pl.semaphore_wait(barrier, devices - 1)

            @pl.when(i > 0)
            def _():
                send(c, i - 1)

            places = [(partner(turn(i * together + n)), c) for n in range(together)]
            for p in range(local_pieces):
                for (k, _), summed in zip(places, windows(places, p)):
                    pooled[k, p, c * rows : (c + 1) * rows, :] = summed

        arrived[c][me] = pooled[me, :, c * rows : (c + 1) * rows, :]
        send(c, devices // together - 1)

    step = next(n for n in (3 * width, width) if wide % n == 0)
    parts = [slice(i, i + step) for i in range(0, wide, step)]
    for load in loads[len(first) :]:
        load.wait()
    out_weight = out_w_ref[...].astype(jnp.float32)[None, :]
    row_at = lax.broadcasted_iota(jnp.int32, (rows, 2 * half), 0)
    column_at = lax.broadcasted_iota(jnp.int32, (rows, 2 * half), 1)

    for c in range(CHUNKS):
        feats[:, :width] = dense_ref[pl.ds(pl.multiple_of(role * half + c * rows, rows), rows), :].astype(jnp.float32)

        @pl.loop(1, devices)
        def _(s):
            there(c, s).wait_recv()

        def piece(index):
            return arrived[c][index // local_pieces, index % local_pieces].astype(jnp.float32)

        @pl.loop(0, tables)
        def _(t):
            def add(e, acc):
                own = plan_ref[tables + spares + e] == t
                return acc + piece(plan_ref[tables + e]) * jnp.where(own, 1.0, 0.0)

            acc = piece(plan_ref[t])
            if spares <= 16:
                for e in range(spares):
                    acc = add(e, acc)
            else:
                acc = lax.fori_loop(0, spares, add, acc)
            feats[:, pl.ds(pl.multiple_of((t + 1) * width, width), width)] = acc

        if c == 0:
            load_u.wait()
        low_rank = dot(feats[...].astype(jnp.bfloat16), u_ref[...]).astype(jnp.bfloat16)
        if c == 0:
            load_v.wait()
            load_w.wait()
        pre_act = b1_ref[...][None, :]
        for part in parts:
            cross_out = dot(low_rank, v_ref[:, part]) + bias_ref[part][None, :]
            crossed[:, part] = cross_out
            own = feats[:, part]
            pre_act = pre_act + dot((own * cross_out + own).astype(jnp.bfloat16), w_ref[part, :])
        sig_act = jax.nn.sigmoid(pre_act)
        logits = jnp.sum(pre_act * sig_act * out_weight, axis=1, keepdims=True)
        labels = jnp.sum(
            jnp.where(row_at + (role * half + c * rows) == column_at, label_ref[...][None, :], 0.0),
            axis=1,
            keepdims=True,
        )
        grad_logit = jax.nn.sigmoid(logits) - labels
        slope = sig_act * (1.0 + pre_act * (1.0 - sig_act))
        grad_act = (grad_logit * out_weight * slope).astype(jnp.bfloat16)
        grad_low = jnp.zeros((rows, u_ref.shape[1]), jnp.float32)
        for part in parts:
            grad_mixed = dot(grad_act, w_ref[part, :], NT)
            grad_cross = (grad_mixed * feats[:, part]).astype(jnp.bfloat16)
            mixed_grad[:, part] = grad_mixed * (crossed[:, part] + 1.0)
            grad_low = grad_low + dot(grad_cross, v_ref[:, part], NT)
        grad_low = grad_low.astype(jnp.bfloat16)
        for part in parts:
            whole = (mixed_grad[:, part] + dot(grad_low, u_ref[part, :], NT)).astype(jnp.bfloat16)
            for i in range(step // width):
                grads[part.start // width + i] = whole[:, i * width : (i + 1) * width]

        @pl.loop(0, devices)
        def _(i):
            d = partner(turn(i))
            for p in range(local_pieces):
                outgoing[c][d, p] = grads[plan_ref[owners + d * local_pieces + p] + 1]

            @pl.when(i > 0)
            def _():
                back(c, turn(i - 1)).start()

        out_ref[me, :, c * rows : (c + 1) * rows, :] = outgoing[c][me]

    for c in range(CHUNKS):

        @pl.loop(1, devices)
        def _(s):
            there(c, s).wait_send()
            back(c, s).wait_send()
            back(c, s).wait_recv()


def local(
    table_rows, piece_table, bag_rows, bag_of, bag_weight, dense_input, labels,
    cross_u, cross_v, cross_bias, top_w1, top_b1, out_w,
):
    devices = lax.axis_size("dev")
    local_pieces, length, width = table_rows.shape
    half = dense_input.shape[0] // 2
    rows = half // CHUNKS
    wide = cross_u.shape[0]
    tables = wide // width - 1

    def tiled(array):
        return array.reshape(local_pieces, -1, LANES).transpose(1, 0, 2)

    bag_rows, bag_of, bag_weight = tiled(bag_rows), tiled(bag_of), tiled(bag_weight)
    plans, base, extra = plan(piece_table, table_rows, bag_rows, bag_of, bag_weight, half, devices, tables)
    vmem = pl.BlockSpec(memory_space=pltpu.VMEM)
    hbm = pl.BlockSpec(memory_space=pltpu.HBM)
    shape = (devices, local_pieces, half, width)
    block = pltpu.VMEM((devices, local_pieces, rows, width), jnp.bfloat16)
    returned = pl.pallas_call(
        step_kernel,
        out_shape=jax.ShapeDtypeStruct(shape, jnp.bfloat16),
        in_specs=[hbm] * 15,
        out_specs=vmem,
        scratch_shapes=[
            pltpu.SMEM(plans.shape, jnp.int32),
            pltpu.SMEM(base.shape, jnp.int32),
            pltpu.VMEM(dense_input.shape, jnp.bfloat16),
            pltpu.VMEM(labels.shape, jnp.float32),
            pltpu.VMEM(cross_bias.shape, jnp.float32),
            pltpu.VMEM(top_b1.shape, jnp.float32),
            pltpu.VMEM(out_w.shape, jnp.bfloat16),
            pltpu.VMEM(bag_of.shape, jnp.int32),
            pltpu.VMEM(bag_rows.shape, jnp.int32),
            pltpu.VMEM(bag_weight.shape, jnp.bfloat16),
            pltpu.VMEM(bag_weight.shape, jnp.float32),
            pltpu.VMEM(table_rows.shape, jnp.bfloat16),
            pltpu.VMEM((local_pieces, length // LOW * width, LOW), jnp.bfloat16),
            pltpu.VMEM(shape, jnp.bfloat16),
            pltpu.VMEM(shape, jnp.bfloat16),
            pltpu.VMEM(cross_u.shape, jnp.bfloat16),
            pltpu.VMEM(cross_v.shape, jnp.bfloat16),
            pltpu.VMEM(top_w1.shape, jnp.bfloat16),
            pltpu.VMEM((rows, wide), jnp.float32),
            pltpu.VMEM((rows, wide), jnp.float32),
            pltpu.VMEM((rows, wide), jnp.float32),
            pltpu.VMEM((wide // width, rows, width), jnp.bfloat16),
            [block] * CHUNKS,
            [block] * CHUNKS,
            pltpu.SemaphoreType.DMA((15,)),
        ]
        + [pltpu.SemaphoreType.DMA((CHUNKS, devices))] * 4,
        compiler_params=pltpu.CompilerParams(
            vmem_limit_bytes=60 * 1024 * 1024, collective_id=0, has_side_effects=True
        ),
    )(
        plans, base, dense_input, labels, cross_bias, top_b1, out_w,
        bag_of, bag_rows, bag_weight, table_rows, extra, cross_u, cross_v, top_w1,
    )
    return returned.transpose(0, 2, 1, 3)


def solution(mesh):
    split, whole = P("dev"), P()
    return jax.shard_map(
        local,
        mesh=mesh,
        in_specs=(split, whole, split, split, split, split, split) + (whole,) * 6,
        out_specs=P(None, "role", "dev", None),
        check_vma=False,
    )
```

```python
import functools

import jax
import jax.numpy as jnp
from jax import lax
from jax.experimental import pallas as pl
from jax.experimental.pallas import tpu as pltpu
from jax.sharding import PartitionSpec as P

LANES = 128
WINDOW = 2 * LANES
LOW = 256
CHUNKS = 2
TOGETHER = 4
NT = (((1,), (1,)), ((), ()))
NN = (((1,), (0,)), ((), ()))


def dot(a, b, dims=NN):
    return lax.dot_general(a, b, dims, preferred_element_type=jnp.float32)


def flip(tile):
    return tile.astype(jnp.float32).T.astype(jnp.bfloat16)


def pick(table, width, ids):
    low_ids = lax.broadcasted_iota(jnp.int32, (LOW, ids.shape[1]), 0)
    low, high = ids % LOW, ids // LOW
    hot = jnp.where(low_ids == low, 1.0, 0.0).astype(jnp.bfloat16)
    picked = dot(table[:width, :], hot)
    for g in range(1, table.shape[0] // width):
        picked = jnp.where(high == g, dot(table[g * width : (g + 1) * width, :], hot), picked)
    return picked.astype(jnp.bfloat16)


def spread_out(bags, scale, rows):
    bag_ids = lax.broadcasted_iota(jnp.int32, (rows, bags.shape[1]), 0)
    return jnp.where(bag_ids == bags, scale, 0.0).astype(jnp.bfloat16)


def plan_kernel(
    tables, owner_ref, bags_hbm, rows_hbm, scale_hbm, table_hbm, plan_ref, base_ref, extra_hbm,
    bags_ref, rows_ref, scale_ref, scale_wide, table_ref, flipped, stage, sems,
):
    blocks, pieces, half, width = extra_hbm.shape
    tiles = bags_ref.shape[0]
    rows = half // CHUNKS
    shift = rows.bit_length() - 1
    spares = max(1, owner_ref.shape[0] - tables)
    flags = tables + 2 * spares
    owners = flags + blocks * pieces * CHUNKS
    role = lax.axis_index("role")
    load_bags = pltpu.make_async_copy(bags_hbm, bags_ref, sems.at[3])
    load_bags.start()

    @pl.loop(0, tables)
    def _(t):
        plan_ref[t] = -1

    @pl.loop(0, spares)
    def _(e):
        plan_ref[tables + e] = 0
        plan_ref[tables + spares + e] = -1

    def assign(p, used):
        t = owner_ref[p]
        plan_ref[owners + p] = t
        again = plan_ref[t] >= 0

        @pl.when(again)
        def _():
            plan_ref[tables + used] = p
            plan_ref[tables + spares + used] = t

        @pl.when(jnp.logical_not(again))
        def _():
            plan_ref[t] = p

        return used + again.astype(jnp.int32)

    lax.fori_loop(0, owner_ref.shape[0], assign, jnp.int32(0))

    @pl.loop(0, owners - flags)
    def _(i):
        plan_ref[flags + i] = 0

    load_bags.wait()

    group = lax.broadcasted_iota(jnp.int32, base_ref.shape, 1)
    edges = (2 * (group // CHUNKS) + role) * half + group % CHUNKS * rows

    ahead = WINDOW // LANES

    def count(t, state):
        base, over = state
        here = bags_ref[t]
        base = base + jnp.where(here[:, LANES - 1 :] < edges, 1, 0)
        same = (here >> shift) == (bags_ref[t + ahead] >> shift)
        return base, jnp.maximum(over, jnp.where(same, 1, 0))

    state = (jnp.zeros(base_ref.shape, jnp.int32), jnp.zeros((pieces, LANES), jnp.int32))
    base, over = lax.fori_loop(0, tiles - ahead, count, state, unroll=True if tiles <= 64 else 8)
    for t in range(tiles - ahead, tiles):
        base = base + jnp.where(bags_ref[t][:, LANES - 1 :] < edges, 1, 0)
    base_ref[...] = jnp.minimum(base, tiles - ahead - 1)

    @pl.when(jnp.max(over) > 0)
    def _():
        loads = [
            pltpu.make_async_copy(rows_hbm, rows_ref, sems.at[0]),
            pltpu.make_async_copy(scale_hbm, scale_ref, sems.at[1]),
            pltpu.make_async_copy(table_hbm, table_ref, sems.at[2]),
        ]
        for load in loads:
            load.start()
        for load in loads:
            load.wait()
        scale_wide[...] = scale_ref[...].astype(jnp.float32)
        for p in range(pieces):
            for g in range(table_ref.shape[1] // LOW):
                flipped[p, g * width : (g + 1) * width, :] = flip(table_ref[p, g * LOW : (g + 1) * LOW, :])

        for p in range(pieces):

            @pl.loop(0, blocks * CHUNKS)
            def _(e):
                k, c = e // CHUNKS, e % CHUNKS
                edge = (2 * k + role) * half + c * rows
                bags = bags_ref[:, p, :]
                first = jnp.sum(jnp.where(bags < edge, 1, 0))
                last = jnp.sum(jnp.where(bags < edge + rows, 1, 0))
                begin = first // LANES

                def more(t, acc):
                    picked = pick(flipped[p], width, rows_ref[t, p : p + 1, :])
                    spread = spread_out(bags_ref[t, p : p + 1, :] - edge, scale_wide[t, p : p + 1, :], rows)
                    return acc + dot(spread, picked, NT)

                @pl.when(last - first > WINDOW)
                def _():
                    plan_ref[flags + (k * pieces + p) * CHUNKS + c] = 1
                    end = (last + LANES - 1) // LANES
                    acc = lax.fori_loop(begin, end, more, jnp.zeros((rows, width), jnp.float32))
                    stage[...] = acc.astype(jnp.bfloat16)
                    put = pltpu.make_async_copy(
                        stage, extra_hbm.at[k, p, pl.ds(pl.multiple_of(c * rows, rows), rows), :], sems.at[0]
                    )
                    put.start()
                    put.wait()


def plan(piece_table, table_rows, bag_rows, bag_of, bag_weight, half, blocks, tables):
    pieces, length, width = table_rows.shape
    spares = max(1, piece_table.shape[0] - tables)
    lanes = -(-blocks * CHUNKS // LANES) * LANES
    entries = tables + 2 * spares + blocks * pieces * CHUNKS + piece_table.shape[0]
    vmem = pl.BlockSpec(memory_space=pltpu.VMEM)
    smem = pl.BlockSpec(memory_space=pltpu.SMEM)
    hbm = pl.BlockSpec(memory_space=pltpu.HBM)
    return pl.pallas_call(
        functools.partial(plan_kernel, tables),
        out_shape=[
            jax.ShapeDtypeStruct((-(-entries // LANES) * LANES,), jnp.int32),
            jax.ShapeDtypeStruct((pieces, lanes), jnp.int32),
            jax.ShapeDtypeStruct((blocks, pieces, half, width), jnp.bfloat16),
        ],
        in_specs=[smem, hbm, hbm, hbm, hbm],
        out_specs=[smem, vmem, hbm],
        scratch_shapes=[
            pltpu.VMEM(bag_of.shape, jnp.int32),
            pltpu.VMEM(bag_rows.shape, jnp.int32),
            pltpu.VMEM(bag_weight.shape, jnp.bfloat16),
            pltpu.VMEM(bag_weight.shape, jnp.float32),
            pltpu.VMEM(table_rows.shape, jnp.bfloat16),
            pltpu.VMEM((pieces, length // LOW * width, LOW), jnp.bfloat16),
            pltpu.VMEM((half // CHUNKS, width), jnp.bfloat16),
            pltpu.SemaphoreType.DMA((4,)),
        ],
        compiler_params=pltpu.CompilerParams(vmem_limit_bytes=60 * 1024 * 1024),
    )(piece_table, bag_of, bag_rows, bag_weight, table_rows)


def step_kernel(
    plan_hbm, base_hbm, dense_hbm, label_hbm, bias_hbm, b1_hbm, out_w_hbm, bags_hbm, rows_hbm, scale_hbm, table_hbm, extra_hbm, u_hbm, v_hbm, w_hbm, out_ref,
    plan_ref, base_ref, dense_ref, label_ref, bias_ref, b1_ref, out_w_ref,
    bags_ref, rows_ref, scale_ref, scale_wide, table_ref, flipped, extra_ref, pooled,
    u_ref, v_ref, w_ref, feats, crossed, mixed_grad, grads, arrived, outgoing,
    sems, there_send, there_recv, back_send, back_recv,
):
    devices, local_pieces, half, width = out_ref.shape
    pieces = devices * local_pieces
    rows, wide = feats.shape
    tables = wide // width - 1
    spares = max(1, pieces - tables)
    flags = tables + 2 * spares
    owners = flags + devices * local_pieces * CHUNKS
    role = lax.axis_index("role")
    me = lax.axis_index("dev")
    first = [
        (table_hbm, table_ref), (scale_hbm, scale_ref), (bags_hbm, bags_ref), (rows_hbm, rows_ref),
        (plan_hbm, plan_ref), (base_hbm, base_ref), (extra_hbm, extra_ref),
    ]
    later = [
        (dense_hbm, dense_ref), (label_hbm, label_ref), (bias_hbm, bias_ref), (b1_hbm, b1_ref), (out_w_hbm, out_w_ref),
    ]
    loads = [pltpu.make_async_copy(*pair, sems.at[3 + n]) for n, pair in enumerate(first + later)]
    load_u = pltpu.make_async_copy(u_hbm, u_ref, sems.at[0])
    load_v = pltpu.make_async_copy(v_hbm, v_ref, sems.at[1])
    load_w = pltpu.make_async_copy(w_hbm, w_ref, sems.at[2])
    barrier = pltpu.get_barrier_semaphore()

    for load in loads:
        load.start()

    @pl.loop(1, devices)
    def _(s):
        pl.semaphore_signal(
            barrier, inc=1, device_id={"dev": (me + s) % devices}, device_id_type=pl.DeviceIdType.MESH
        )

    load_u.start()
    load_v.start()
    load_w.start()

    def partner(s):
        if devices & (devices - 1):
            return (me + s) % devices
        peer = 0
        for b in range(devices.bit_length() - 1):
            bit = 1 << b
            peer = peer + bit * ((me // bit + s // bit) % 2)
        return peer

    def there(c, s):
        peer = partner(s)
        return pltpu.make_async_remote_copy(
            src_ref=pooled.at[peer, :, c * rows : (c + 1) * rows, :],
            dst_ref=arrived[c].at[me],
            send_sem=there_send.at[c, s],
            recv_sem=there_recv.at[c, s],
            device_id={"dev": peer},
            device_id_type=pl.DeviceIdType.MESH,
        )

    def keep(c):
        return pltpu.make_async_copy(
            outgoing[c].at[me], out_ref.at[me, :, c * rows : (c + 1) * rows, :], sems.at[15 + c]
        )

    def back(c, s):
        peer = partner(s)
        return pltpu.make_async_remote_copy(
            src_ref=outgoing[c].at[peer],
            dst_ref=out_ref.at[me, :, c * rows : (c + 1) * rows, :],
            send_sem=back_send.at[c, s],
            recv_sem=back_recv.at[c, s],
            device_id={"dev": peer},
            device_id_type=pl.DeviceIdType.MESH,
        )

    loads[0].wait()
    for p in range(local_pieces):
        for g in range(table_ref.shape[1] // LOW):
            flipped[p, g * width : (g + 1) * width, :] = flip(table_ref[p, g * LOW : (g + 1) * LOW, :])
    for load in loads[1 : len(first)]:
        load.wait()
    scale_wide[...] = scale_ref[...].astype(jnp.float32)

    def windows(places, p):
        laid = []
        for k, c in places:
            edge = (2 * k + role) * half + c * rows
            at = base_ref[p, k * CHUNKS + c]

            def tiles(ref):
                return [ref[at + j, p : p + 1, :] for j in range(WINDOW // LANES + 1)]

            bags = tiles(bags_ref)
            early = bags[0] < edge

            def lay(tiles):
                return [jnp.where(early, tiles[-1], tiles[0])] + tiles[1:-1]

            laid.append((lay(tiles(rows_ref)), [bag - edge for bag in lay(bags)], lay(tiles(scale_wide))))
        picked = pick(flipped[p], width, jnp.concatenate([tile for ids, _, _ in laid for tile in ids], axis=1))
        sums = []
        for n, (k, c) in enumerate(places):
            bags, scale = (jnp.concatenate(tiles, axis=1) for tiles in laid[n][1:])
            summed = dot(spread_out(bags, scale, rows), picked[:, n * WINDOW : (n + 1) * WINDOW], NT)
            flag = jnp.zeros((rows, width), jnp.int32) + plan_ref[flags + (k * local_pieces + p) * CHUNKS + c]
            other = extra_ref[k, p, c * rows : (c + 1) * rows, :].astype(jnp.float32)
            sums.append(jnp.where(flag > 0, other, summed).astype(jnp.bfloat16))
        return sums

    together = TOGETHER if devices % TOGETHER == 0 else 1

    def turn(i):
        return devices - 1 - i

    def send(c, i):
        for n in range(together):
            s = turn(i * together + n)

            @pl.when(s > 0)
            def _():
                there(c, s).start()

    for c in range(CHUNKS):

        @pl.loop(0, devices // together)
        def _(i):
            if c == 0:

                @pl.when(i == 1)
                def _():
                    pl.semaphore_wait(barrier, devices - 1)

            @pl.when(i > 0)
            def _():
                send(c, i - 1)

            places = [(partner(turn(i * together + n)), c) for n in range(together)]
            for p in range(local_pieces):
                for (k, _), summed in zip(places, windows(places, p)):
                    pooled[k, p, c * rows : (c + 1) * rows, :] = summed

        arrived[c][me] = pooled[me, :, c * rows : (c + 1) * rows, :]
        send(c, devices // together - 1)

    step = next(n for n in (3 * width, width) if wide % n == 0)
    parts = [slice(i, i + step) for i in range(0, wide, step)]
    for load in loads[len(first) :]:
        load.wait()
    out_weight = out_w_ref[...].astype(jnp.float32)[None, :]
    row_at = lax.broadcasted_iota(jnp.int32, (rows, 2 * half), 0)
    column_at = lax.broadcasted_iota(jnp.int32, (rows, 2 * half), 1)

    for c in range(CHUNKS):
        feats[:, :width] = dense_ref[pl.ds(pl.multiple_of(role * half + c * rows, rows), rows), :].astype(jnp.float32)

        @pl.loop(1, devices)
        def _(s):
            there(c, s).wait_recv()

        def piece(index):
            return arrived[c][index // local_pieces, index % local_pieces].astype(jnp.float32)

        @pl.loop(0, tables)
        def _(t):
            def add(e, acc):
                own = plan_ref[tables + spares + e] == t
                return acc + piece(plan_ref[tables + e]) * jnp.where(own, 1.0, 0.0)

            acc = piece(plan_ref[t])
            if spares <= 16:
                for e in range(spares):
                    acc = add(e, acc)
            else:
                acc = lax.fori_loop(0, spares, add, acc)
            feats[:, pl.ds(pl.multiple_of((t + 1) * width, width), width)] = acc

        if c == 0:
            load_u.wait()
        low_rank = dot(feats[...].astype(jnp.bfloat16), u_ref[...]).astype(jnp.bfloat16)
        if c == 0:
            load_v.wait()
            load_w.wait()
        pre_act = b1_ref[...][None, :]
        for part in parts:
            cross_out = dot(low_rank, v_ref[:, part]) + bias_ref[part][None, :]
            crossed[:, part] = cross_out
            own = feats[:, part]
            pre_act = pre_act + dot((own * cross_out + own).astype(jnp.bfloat16), w_ref[part, :])
        sig_act = jax.nn.sigmoid(pre_act)
        logits = jnp.sum(pre_act * sig_act * out_weight, axis=1, keepdims=True)
        labels = jnp.sum(
            jnp.where(row_at + (role * half + c * rows) == column_at, label_ref[...][None, :], 0.0),
            axis=1,
            keepdims=True,
        )
        grad_logit = jax.nn.sigmoid(logits) - labels
        slope = sig_act * (1.0 + pre_act * (1.0 - sig_act))
        grad_act = (grad_logit * out_weight * slope).astype(jnp.bfloat16)
        grad_low = jnp.zeros((rows, u_ref.shape[1]), jnp.float32)
        for part in parts:
            grad_mixed = dot(grad_act, w_ref[part, :], NT)
            grad_cross = (grad_mixed * feats[:, part]).astype(jnp.bfloat16)
            mixed_grad[:, part] = grad_mixed * (crossed[:, part] + 1.0)
            grad_low = grad_low + dot(grad_cross, v_ref[:, part], NT)
        grad_low = grad_low.astype(jnp.bfloat16)
        for part in parts:
            whole = (mixed_grad[:, part] + dot(grad_low, u_ref[part, :], NT)).astype(jnp.bfloat16)
            for i in range(step // width):
                grads[part.start // width + i] = whole[:, i * width : (i + 1) * width]

        @pl.loop(0, devices)
        def _(i):
            d = partner(turn(i))
            for p in range(local_pieces):
                outgoing[c][d, p] = grads[plan_ref[owners + d * local_pieces + p] + 1]

            @pl.when(i > 0)
            def _():
                back(c, turn(i - 1)).start()

        keep(c).start()

    for c in range(CHUNKS):
        keep(c).wait()

        @pl.loop(1, devices)
        def _(s):
            there(c, s).wait_send()
            back(c, s).wait_send()
            back(c, s).wait_recv()


def local(
    table_rows, piece_table, bag_rows, bag_of, bag_weight, dense_input, labels,
    cross_u, cross_v, cross_bias, top_w1, top_b1, out_w,
):
    devices = lax.axis_size("dev")
    local_pieces, length, width = table_rows.shape
    half = dense_input.shape[0] // 2
    rows = half // CHUNKS
    wide = cross_u.shape[0]
    tables = wide // width - 1

    def tiled(array):
        return array.reshape(local_pieces, -1, LANES).transpose(1, 0, 2)

    bag_rows, bag_of, bag_weight = tiled(bag_rows), tiled(bag_of), tiled(bag_weight)
    plans, base, extra = plan(piece_table, table_rows, bag_rows, bag_of, bag_weight, half, devices, tables)
    hbm = pl.BlockSpec(memory_space=pltpu.HBM)
    shape = (devices, local_pieces, half, width)
    block = pltpu.VMEM((devices, local_pieces, rows, width), jnp.bfloat16)
    returned = pl.pallas_call(
        step_kernel,
        out_shape=jax.ShapeDtypeStruct(shape, jnp.bfloat16),
        in_specs=[hbm] * 15,
        out_specs=hbm,
        scratch_shapes=[
            pltpu.SMEM(plans.shape, jnp.int32),
            pltpu.SMEM(base.shape, jnp.int32),
            pltpu.VMEM(dense_input.shape, jnp.bfloat16),
            pltpu.VMEM(labels.shape, jnp.float32),
            pltpu.VMEM(cross_bias.shape, jnp.float32),
            pltpu.VMEM(top_b1.shape, jnp.float32),
            pltpu.VMEM(out_w.shape, jnp.bfloat16),
            pltpu.VMEM(bag_of.shape, jnp.int32),
            pltpu.VMEM(bag_rows.shape, jnp.int32),
            pltpu.VMEM(bag_weight.shape, jnp.bfloat16),
            pltpu.VMEM(bag_weight.shape, jnp.float32),
            pltpu.VMEM(table_rows.shape, jnp.bfloat16),
            pltpu.VMEM((local_pieces, length // LOW * width, LOW), jnp.bfloat16),
            pltpu.VMEM(shape, jnp.bfloat16),
            pltpu.VMEM(shape, jnp.bfloat16),
            pltpu.VMEM(cross_u.shape, jnp.bfloat16),
            pltpu.VMEM(cross_v.shape, jnp.bfloat16),
            pltpu.VMEM(top_w1.shape, jnp.bfloat16),
            pltpu.VMEM((rows, wide), jnp.float32),
            pltpu.VMEM((rows, wide), jnp.float32),
            pltpu.VMEM((rows, wide), jnp.float32),
            pltpu.VMEM((wide // width, rows, width), jnp.bfloat16),
            [block] * CHUNKS,
            [block] * CHUNKS,
            pltpu.SemaphoreType.DMA((15 + CHUNKS,)),
        ]
        + [pltpu.SemaphoreType.DMA((CHUNKS, devices))] * 4,
        compiler_params=pltpu.CompilerParams(
            vmem_limit_bytes=60 * 1024 * 1024, collective_id=0, has_side_effects=True
        ),
    )(
        plans, base, dense_input, labels, cross_bias, top_b1, out_w,
        bag_of, bag_rows, bag_weight, table_rows, extra, cross_u, cross_v, top_w1,
    )
    return returned.transpose(0, 2, 1, 3)


def solution(mesh):
    split, whole = P("dev"), P()
    return jax.shard_map(
        local,
        mesh=mesh,
        in_specs=(split, whole, split, split, split, split, split) + (whole,) * 6,
        out_specs=P(None, "role", "dev", None),
        check_vma=False,
    )
```
